32 devices in a mesh: parts: 2 (over x), shot: 2 (over core), space: 8 (over z, y).
Axes of the slice: x: 2, y: 2, z: 4, core: 2. Of those that a mesh axis runs over, the one named last changes fastest.
Arguments:
- image: float32 [3200, 2, 192], P(('parts', 'space')), parts along dimension 0, may hold values from -6 to 6
- coil_maps: bfloat16 [16, 3200, 2, 192], P(None, ('parts', 'space')), parts along dimension 1, may hold values from -1.5 to 1.5
- psf_phase: float32 [3200, 576], P(('parts', 'space')), parts along dimension 0, may hold values from -3.140625 to 3.140625
- line_mask: int32 [4, 200], P(('parts', 'shot')), parts along dimension 0, may hold values 0 or 1
- motion: int32 [4, 3], P(('parts', 'shot')), parts along dimension 0, may hold values from 0 to 16
Outputs:
- result: float32 [3200, 2, 192], P(('parts', 'space')), parts along dimension 0
The draws below stay inside these ranges and needn't reach their ends.
There are 2 independent parts, one for each index of `parts`. The reference program is written for one: setup_inputs(seed, part) draws one part's arguments, and reference() takes and returns one part's arrays. A program takes and returns all parts, laid end to end along the dimension named above; each array names one. Nothing has to cross between parts.
Inputs may be any that keep to these rules, and one draw needn't show every extreme that they name: `motion`: column 0 selects the rotation angle, columns 1 and 2 the shifts along x and y.
All inputs are finite; a program needn't handle non-finite values. No bound on the sum of `line_mask` on one device may be relied on, other than what follows from the above.
Results may differ from the reference program's by a relative error of at most 0.003.
Values may be sent and summed in bfloat16 or wider, within the bound.
A program may use at most 64 MiB of HBM per device.

```python
import jax
import jax.numpy as jnp
from jax import lax

NX = 192
NY = 200
COILS = 16
Z = 8
LEVELS = 17
NR = 576
SHOTS = 2


def place_ends(entries, key, smallest, high):
    spot = [jax.random.randint(jax.random.fold_in(key, axis), (), 0, length) for axis, length in enumerate(entries.shape)]
    widest = entries.shape.index(max(entries.shape))
    beside = spot[:widest] + [(spot[widest] + 1) % entries.shape[widest]] + spot[widest + 1:]
    return entries.at[tuple(spot)].set(smallest).at[tuple(beside)].set(high)


def level_of(own_key, shape, split, smallest, top_value):
    def one(axis_at, blocks):
        heights = jax.random.uniform(jax.random.fold_in(jax.random.fold_in(own_key, 6), axis_at), (blocks,), jnp.float32, smallest / len(split), top_value / len(split))
        return jnp.repeat(jnp.exp(heights), shape[axis_at] // blocks).reshape((-1,) + (1,) * (len(shape) - axis_at - 1))

    factor_of = one(*split[0])
    for cut in split[1:]:
        factor_of = factor_of * one(*cut)
    return factor_of


def scatter_about(key, extent, deviation, most, cuts=(), held_as=jnp.bfloat16):
    entries = deviation * jax.random.normal(key, extent, jnp.float32)
    if cuts:
        entries = entries * level_of(key, extent, cuts, -0.22, 0.18)
    return jnp.clip(entries, -most, most).astype(held_as)


def setup_inputs(seed: int = 0, part: int = 0) -> dict:
    splits = jax.random.split(jax.random.key(seed), 6)
    own_keys = jax.random.split(jax.random.fold_in(splits[5], part), 6)
    image = scatter_about(own_keys[0], (Z * NY, 2, NX), 1.0, 6.0, ((0, 8),), jnp.float32)
    coil_maps = scatter_about(own_keys[1], (COILS, Z * NY, 2, NX), COILS ** -0.5, 1.5, ((1, 8),))
    psf_phase = jnp.clip(jax.random.uniform(own_keys[2], (Z * NY, NR), jnp.float32, -3.140625, 3.140625), -3.140625, 3.140625)
    line_mask = place_ends((jax.random.randint(own_keys[3], (SHOTS, NY), 0, 3) < 1).astype(jnp.int32), jax.random.fold_in(own_keys[3], 1), 0, 1)
    motion = place_ends(jax.random.randint(own_keys[4], (SHOTS, 3), 0, LEVELS), jax.random.fold_in(own_keys[4], 1), 0, LEVELS - 1).astype(jnp.int32)
    return dict(image=image, coil_maps=coil_maps, psf_phase=psf_phase, line_mask=line_mask, motion=motion)


PRECISE = lax.Precision.HIGHEST
ANGLE_STEP = 0.02
SHIFT_STEP = 0.5


def dft_parts(size_in, size_out, modulus, sign):
    inputs = jnp.arange(size_in, dtype=jnp.int32)[:, None]
    outputs = jnp.arange(size_out, dtype=jnp.int32)[None, :]
    angle = ((inputs * outputs) % modulus).astype(jnp.float32) * (2.0 * jnp.pi / modulus)
    factor = float(modulus) ** -0.5
    return jnp.cos(angle) * factor, jnp.sin(angle) * (sign * factor)


def block(parts):
    real_part, imag_part = parts
    upper = jnp.concatenate([real_part, imag_part], 1)
    bottom = jnp.concatenate([-imag_part, real_part], 1)
    return jnp.concatenate([upper, bottom], 0)


def quad(real_part, imag_part):
    return jnp.stack([jnp.stack([real_part, -imag_part], 1), jnp.stack([imag_part, real_part], 1)], 0)


def signed_freq(length):
    counter = jnp.arange(length, dtype=jnp.int32)
    return jnp.where(counter < length // 2, counter, counter - length).astype(jnp.float32)


def turn_phase(values, phase):
    cosine = jnp.cos(phase)
    sine_part = jnp.sin(phase)
    real_part = values[..., 0, :]
    imag_part = values[..., 1, :]
    return jnp.stack([real_part * cosine - imag_part * sine_part, real_part * sine_part + imag_part * cosine], -2)


def complex_mul(left, right):
    return jnp.stack([left[..., 0, :] * right[..., 0, :] - left[..., 1, :] * right[..., 1, :],
                      left[..., 0, :] * right[..., 1, :] + left[..., 1, :] * right[..., 0, :]], -2)


def conj_mul(left, right):
    return jnp.stack([left[..., 0, :] * right[..., 0, :] + left[..., 1, :] * right[..., 1, :],
                      left[..., 0, :] * right[..., 1, :] - left[..., 1, :] * right[..., 0, :]], -2)


def shear_rows(values, shift, sign):
    length = values.shape[-1]
    lines = values.shape[0]
    forward = block(dft_parts(length, length, length, -1.0))
    inverse = block(dft_parts(length, length, length, 1.0))
    spectra = jnp.dot(values.reshape(lines, 2 * length), forward, precision=PRECISE, preferred_element_type=jnp.float32)
    phase = (sign * -2.0 * jnp.pi / length) * shift[:, None] * signed_freq(length)[None, :]
    spectra = turn_phase(spectra.reshape(lines, 2, length), phase)
    result = jnp.dot(spectra.reshape(lines, 2 * length), inverse, precision=PRECISE, preferred_element_type=jnp.float32)
    return result.reshape(lines, 2, length)


def shear_columns(values, shift, sign):
    length = values.shape[1]
    forward = quad(*dft_parts(length, length, length, -1.0))
    inverse = quad(*dft_parts(length, length, length, 1.0))
    spectra = jnp.einsum("oaib,zbix->zaox", forward, values, precision=PRECISE)
    phase = (sign * -2.0 * jnp.pi / length) * signed_freq(length)[:, None] * shift[None, :]
    spectra = turn_phase(spectra, phase)
    return jnp.einsum("oaib,zbix->zaox", inverse, spectra, precision=PRECISE)


def geometry(motion_row):
    offsets = motion_row.astype(jnp.float32) - (LEVELS - 1) / 2.0
    angle = offsets[0] * ANGLE_STEP
    return -jnp.tan(angle / 2.0), jnp.sin(angle), offsets[1] * SHIFT_STEP, offsets[2] * SHIFT_STEP


def rotate(values, motion_row, sign):
    slope, tilt, shift_x, shift_y = geometry(motion_row)
    lines = values.shape[0]
    width = values.shape[2]
    across = (jnp.arange(lines, dtype=jnp.int32) % NY).astype(jnp.float32) - NY / 2.0
    along = jnp.arange(width, dtype=jnp.int32).astype(jnp.float32) - width / 2.0

    def column_pass(current):
        view_slices = current.reshape(lines // NY, NY, 2, width)
        return shear_columns(view_slices, tilt * along + shift_y, sign).reshape(lines, 2, width)

    if sign > 0:
        current = shear_rows(values, slope * across + shift_x, 1.0)
        current = column_pass(current)
        return shear_rows(current, slope * across, 1.0)
    current = shear_rows(values, slope * across, -1.0)
    current = column_pass(current)
    return shear_rows(current, slope * across + shift_x, -1.0)


def line_table(mask_row):
    cosine, sine_part = dft_parts(NY, NY, NY, 1.0)
    weight = mask_row.astype(jnp.float32)[:, None]
    real_part = jnp.dot(cosine.T, weight * cosine, precision=PRECISE) + jnp.dot(sine_part.T, weight * sine_part, precision=PRECISE)
    imag_part = jnp.dot(sine_part.T, weight * cosine, precision=PRECISE) - jnp.dot(cosine.T, weight * sine_part, precision=PRECISE)
    return quad(real_part, imag_part).astype(jnp.bfloat16)


def reference(image, coil_maps, psf_phase, line_mask, motion):
    lines = image.shape[0]
    width = image.shape[2]
    readout = psf_phase.shape[1]
    pad_table = block(dft_parts(width, readout, readout, -1.0)).astype(jnp.bfloat16)
    crop_table = block(dft_parts(readout, width, readout, 1.0)).astype(jnp.bfloat16)

    def one_shot(running, inputs):
        mask_row, motion_row = inputs
        projector = line_table(mask_row).astype(jnp.float32)
        rotated = rotate(image, motion_row, 1)

        def one_coil(combined, coil):
            coil_values = coil.astype(jnp.float32)
            coil_image = complex_mul(coil_values, rotated).astype(jnp.bfloat16)
            spectra = jnp.dot(coil_image.reshape(lines, 2 * width), pad_table, preferred_element_type=jnp.float32)
            waved = turn_phase(spectra.reshape(lines, 2, readout), psf_phase).astype(jnp.bfloat16)
            view_slices = waved.reshape(lines // NY, NY, 2, readout).astype(jnp.float32)
            projected = jnp.einsum("oaib,zbik->zaok", projector, view_slices, precision=PRECISE).astype(jnp.bfloat16)
            unwaved = turn_phase(projected.reshape(lines, 2, readout).astype(jnp.float32), -psf_phase).astype(jnp.bfloat16)
            back = jnp.dot(unwaved.reshape(lines, 2 * readout), crop_table, preferred_element_type=jnp.float32)
            return combined + conj_mul(coil_values, back.reshape(lines, 2, width)), None

        combined, _ = lax.scan(one_coil, jnp.zeros(image.shape, jnp.float32), coil_maps)
        return running + rotate(combined, motion_row, -1), None

    result, _ = lax.scan(one_shot, jnp.zeros(image.shape, jnp.float32), (line_mask, motion))
    return result
```

```python
import functools
import math

import jax
import jax.numpy as jnp
import numpy as np
from jax import lax
from jax.experimental import pallas as pl
from jax.experimental.pallas import tpu as pltpu
from jax.sharding import PartitionSpec as P

NY = 200
LEVELS = 17


PRECISE = lax.Precision.HIGHEST
ANGLE_STEP = 0.02
SHIFT_STEP = 0.5


def from_partner(value, axis, apart):
    mask = 2**apart
    pairs = [(source, source ^ mask) for source in range(lax.axis_size(axis))]
    return lax.ppermute(value, axis, pairs)


def dft_parts(size_in, size_out, modulus, sign):
    inputs = jnp.arange(size_in, dtype=jnp.int32)[:, None]
    outputs = jnp.arange(size_out, dtype=jnp.int32)[None, :]
    angle = (inputs * outputs % modulus).astype(jnp.float32) * (2.0 * jnp.pi / modulus)
    factor = float(modulus) ** (-0.5)
    return (jnp.cos(angle) * factor, jnp.sin(angle) * (sign * factor))


def block(parts):
    real_part, imag_part = parts
    upper = jnp.concatenate([real_part, imag_part], 1)
    bottom = jnp.concatenate([-imag_part, real_part], 1)
    return jnp.concatenate([upper, bottom], 0)


def quad(real_part, imag_part):
    return jnp.stack(
        [jnp.stack([real_part, -imag_part], 1), jnp.stack([imag_part, real_part], 1)], 0
    )


def signed_freq(length):
    counter = jnp.arange(length, dtype=jnp.int32)
    return jnp.where(counter < length // 2, counter, counter - length).astype(jnp.float32)


def turn_phase(values, phase):
    cosine = jnp.cos(phase)
    sine_part = jnp.sin(phase)
    real_part = values[..., 0, :]
    imag_part = values[..., 1, :]
    return jnp.stack(
        [real_part * cosine - imag_part * sine_part, real_part * sine_part + imag_part * cosine], -2
    )


def complex_mul(left, right):
    return jnp.stack(
        [
            left[..., 0, :] * right[..., 0, :] - left[..., 1, :] * right[..., 1, :],
            left[..., 0, :] * right[..., 1, :] + left[..., 1, :] * right[..., 0, :],
        ],
        -2,
    )


def conj_mul(left, right):
    return jnp.stack(
        [
            left[..., 0, :] * right[..., 0, :] + left[..., 1, :] * right[..., 1, :],
            left[..., 0, :] * right[..., 1, :] - left[..., 1, :] * right[..., 0, :],
        ],
        -2,
    )


def shear_rows(values, shift, sign):
    length = values.shape[-1]
    lines = values.shape[0]
    forward = block(dft_parts(length, length, length, -1.0))
    inverse = block(dft_parts(length, length, length, 1.0))
    spectra = jnp.dot(
        values.reshape(lines, 2 * length),
        forward,
        precision=PRECISE,
        preferred_element_type=jnp.float32,
    )
    phase = sign * -2.0 * jnp.pi / length * shift[:, None] * signed_freq(length)[None, :]
    spectra = turn_phase(spectra.reshape(lines, 2, length), phase)
    result = jnp.dot(
        spectra.reshape(lines, 2 * length),
        inverse,
        precision=PRECISE,
        preferred_element_type=jnp.float32,
    )
    return result.reshape(lines, 2, length)


def shear_columns(values, shift, sign):
    length = values.shape[1]
    forward = quad(*dft_parts(length, length, length, -1.0))
    inverse = quad(*dft_parts(length, length, length, 1.0))
    spectra = jnp.einsum("oaib,zbix->zaox", forward, values, precision=PRECISE)
    phase = sign * -2.0 * jnp.pi / length * signed_freq(length)[:, None] * shift[None, :]
    spectra = turn_phase(spectra, phase)
    return jnp.einsum("oaib,zbix->zaox", inverse, spectra, precision=PRECISE)


def geometry(motion_row):
    offsets = motion_row.astype(jnp.float32) - (LEVELS - 1) / 2.0
    angle = offsets[0] * ANGLE_STEP
    return (-jnp.tan(angle / 2.0), jnp.sin(angle), offsets[1] * SHIFT_STEP, offsets[2] * SHIFT_STEP)


def line_table(mask_row):
    cosine, sine_part = dft_parts(NY, NY, NY, 1.0)
    weight = mask_row.astype(jnp.float32)[:, None]
    real_part = jnp.dot(cosine.T, weight * cosine, precision=PRECISE) + jnp.dot(
        sine_part.T, weight * sine_part, precision=PRECISE
    )
    imag_part = jnp.dot(sine_part.T, weight * cosine, precision=PRECISE) - jnp.dot(
        cosine.T, weight * sine_part, precision=PRECISE
    )
    return quad(real_part, imag_part).astype(jnp.bfloat16)


def to_columns(values):
    return lax.all_to_all(values, "space", split_axis=2, concat_axis=0, tiled=True)


def to_rows(values):
    return lax.all_to_all(values, "space", split_axis=0, concat_axis=2, tiled=True)


def rotate_shards(values, motion_row, sign, device_rank, devices):
    slope, tilt, shift_x, shift_y = geometry(motion_row)
    lines = values.shape[0]
    width = values.shape[2]
    across = ((device_rank * lines + jnp.arange(lines, dtype=jnp.int32)) % NY).astype(
        jnp.float32
    ) - NY / 2.0

    def column_pass(current):
        columns = width // devices
        along = (device_rank * columns + jnp.arange(columns, dtype=jnp.int32)).astype(
            jnp.float32
        ) - width / 2.0
        gathered = to_columns(current)
        all_lines = gathered.shape[0]
        view_slices = gathered.reshape(all_lines // NY, NY, 2, columns)
        sheared = shear_columns(view_slices, tilt * along + shift_y, sign).reshape(
            all_lines, 2, columns
        )
        return to_rows(sheared)

    if sign > 0:
        current = shear_rows(values, slope * across + shift_x, 1.0)
        current = column_pass(current)
        return shear_rows(current, slope * across, 1.0)
    current = shear_rows(values, slope * across, -1.0)
    current = column_pass(current)
    return shear_rows(current, slope * across + shift_x, -1.0)


def gather_slice(values, bit_count, device_rank):
    for bit_index in range(bit_count):
        partner = from_partner(values, "space", bit_index)
        low_side = device_rank >> bit_index & 1 == 0
        values = jnp.where(
            low_side, jnp.concatenate([values, partner], 0), jnp.concatenate([partner, values], 0)
        )
    return values


def sum_slice(values, bit_count, device_rank):
    for bit_index in reversed(range(bit_count)):
        half_rows = values.shape[0] // 2
        low_side = device_rank >> bit_index & 1 == 0
        kept_part = jnp.where(low_side, values[:half_rows], values[half_rows:])
        sent_part = jnp.where(low_side, values[half_rows:], values[:half_rows])
        values = kept_part + from_partner(sent_part, "space", bit_index)
    return values


def regroup_coils(coil_maps, bit_count, device_rank):
    group_size = 1 << bit_count
    pieces = coil_maps.reshape((group_size, coil_maps.shape[0] // group_size) + coil_maps.shape[1:])
    for bit_index in range(bit_count):
        old_shape = pieces.shape
        halves = pieces.reshape((group_size >> bit_index + 1, 2, 1 << bit_index) + old_shape[1:])
        low_side = device_rank >> bit_index & 1 == 0
        kept_part = jnp.where(low_side, halves[:, 0], halves[:, 1])
        sent_part = jnp.where(low_side, halves[:, 1], halves[:, 0])
        partner = from_partner(sent_part, "space", bit_index)
        pieces = jnp.stack(
            [jnp.where(low_side, kept_part, partner), jnp.where(low_side, partner, kept_part)], 1
        ).reshape(old_shape)
    moved = jnp.moveaxis(pieces, 0, 1)
    return moved.reshape((moved.shape[0], group_size * coil_maps.shape[1]) + coil_maps.shape[2:])


def encode(coils, slab_image, psf_values, pad_table):
    coil_count, lines, _, width = coils.shape
    readout = psf_values.shape[1]
    coil_image = complex_mul(coils.astype(jnp.float32), slab_image[None]).astype(jnp.bfloat16)
    spectra = jnp.dot(
        coil_image.reshape(coil_count * lines, 2 * width),
        pad_table,
        preferred_element_type=jnp.float32,
    )
    return turn_phase(spectra.reshape(coil_count, lines, 2, readout), psf_values[None]).astype(
        jnp.bfloat16
    )


def project(projector, waved):
    coil_count, lines, _, columns = waved.shape
    view_slices = waved.reshape(coil_count, lines // NY, NY, 2, columns)
    projected = jnp.einsum(
        "oaib,czbik->czaok", projector, view_slices, preferred_element_type=jnp.float32
    )
    return projected.astype(jnp.bfloat16).reshape(waved.shape)


def decode(coils, projected, psf_values, crop_table):
    coil_count, lines, _, readout = projected.shape
    width = coils.shape[3]
    unwaved = turn_phase(projected.astype(jnp.float32), -psf_values[None]).astype(jnp.bfloat16)
    back = jnp.dot(
        unwaved.reshape(coil_count * lines, 2 * readout),
        crop_table,
        preferred_element_type=jnp.float32,
    )
    return jnp.sum(
        conj_mul(coils.astype(jnp.float32), back.reshape(coil_count, lines, 2, width)), 0
    )


def round_up(size, step):
    return -(-size // step) * step


def host_dft(size_in, size_out, modulus):
    turns = np.outer(np.arange(size_in), np.arange(size_out)) % modulus
    angle = turns.astype(np.float64) * (2.0 * np.pi / modulus)
    factor = float(modulus) ** -0.5
    return np.cos(angle) * factor, np.sin(angle) * factor


def placed(table, rows, columns):
    out = np.zeros((rows, columns), np.float64)
    out[: table.shape[0], : table.shape[1]] = table
    return out


def split_table(table):
    high = table.astype(np.float32).astype(jnp.bfloat16)
    low = (table - high.astype(np.float64)).astype(np.float32).astype(jnp.bfloat16)
    return np.stack([high, low])


def host_tables(width, height, readout):
    wide, tall, deep = round_up(width, 256), round_up(height, 256), round_up(readout, 128)
    cosine, sine = host_dft(width, readout, readout)
    pad = np.concatenate([placed(cosine, width, deep), placed(sine, width, deep)], 1)
    crop = np.concatenate([placed(cosine.T, deep, wide), placed(sine.T, deep, wide)], 1)
    row_parts = [placed(part, wide, wide) for part in host_dft(width, width, width)]
    column_parts = [placed(part, tall, tall) for part in host_dft(height, height, height)]
    return (
        pad.astype(np.float32).astype(jnp.bfloat16),
        crop.astype(np.float32).astype(jnp.bfloat16),
        split_table(np.concatenate(row_parts, 1)),
        split_table(np.stack(column_parts)),
    )


SINE = [(-1.0) ** n / math.factorial(2 * n + 1) for n in range(6)]
COSINE = [(-1.0) ** n / math.factorial(2 * n) for n in range(7)]


def poly(square, coefficients):
    value = jnp.full_like(square, coefficients[-1])
    for coefficient in reversed(coefficients[:-1]):
        value = value * square + coefficient
    return value


def cos_sin_of_half(half):
    square = half * half
    sine = half * poly(square, SINE)
    cosine = poly(square, COSINE)
    return 1.0 - 2.0 * sine * sine, 2.0 * sine * cosine


def cos_sin_turns(turns):
    rest = turns - jnp.floor(turns + 0.5)
    return cos_sin_of_half(rest * math.pi)


def split_value(value):
    high = value.astype(jnp.bfloat16)
    return high, (value - high.astype(jnp.float32)).astype(jnp.bfloat16)


def mxu(left, right):
    return jnp.dot(left, right, preferred_element_type=jnp.float32)


def slice_kernel(
    height,
    width,
    readout,
    motion_ref,
    mask_ref,
    image_ref,
    coil_ref,
    psf_ref,
    pad_ref,
    crop_ref,
    row_ref,
    column_ref,
    out_ref,
    pad_s,
    crop_s,
    cosine_s,
    sine_s,
    table_s,
    waved_s,
    unwaved_s,
    rotated_s,
    sum_s,
    phase_s,
):
    rows, wide = image_ref.shape[1:]
    deep = cosine_s.shape[1]
    tall = column_ref.shape[2]
    coils = coil_ref.shape[0]

    pad_s[...] = jnp.zeros_like(pad_s)
    pad_s[0:width, :deep] = pad_ref[:, :deep]
    pad_s[0:width, deep:] = -pad_ref[:, deep:]
    pad_s[wide : wide + width, :deep] = pad_ref[:, deep:]
    pad_s[wide : wide + width, deep:] = pad_ref[:, :deep]
    crop_s[0:deep, :] = crop_ref[...]
    crop_s[deep:, :wide] = -crop_ref[:, wide:]
    crop_s[deep:, wide:] = crop_ref[:, :wide]

    cosine_s[...] = jnp.zeros_like(cosine_s)
    sine_s[...] = jnp.zeros_like(sine_s)
    turn_cosine, turn_sine = cos_sin_of_half(psf_ref[...] * 0.5)
    cosine_s[:height, :readout] = turn_cosine
    sine_s[:height, :readout] = turn_sine

    theta = (motion_ref[0, 0].astype(jnp.float32) - (LEVELS - 1) / 2.0) * ANGLE_STEP
    shift_x = (motion_ref[0, 1].astype(jnp.float32) - (LEVELS - 1) / 2.0) * SHIFT_STEP
    shift_y = (motion_ref[0, 2].astype(jnp.float32) - (LEVELS - 1) / 2.0) * SHIFT_STEP
    half = theta * 0.5
    half_square = half * half
    slope = -half * (
        1.0
        + half_square
        * (1.0 / 3.0 + half_square * (2.0 / 15.0 + half_square * (17.0 / 315.0)))
    )
    square = theta * theta
    tilt = theta * (
        1.0 - square * (1.0 / 6.0 - square * (1.0 / 120.0 - square * (1.0 / 5040.0)))
    )

    line = lax.broadcasted_iota(jnp.int32, (rows, wide), 0)
    place = lax.broadcasted_iota(jnp.int32, (rows, wide), 1)
    across = line.astype(jnp.float32) - height / 2.0
    along = place.astype(jnp.float32) - width / 2.0
    place_freq = jnp.where(place < width // 2, place, place - width).astype(jnp.float32) / width
    line_freq = jnp.where(line < height // 2, line, line - height).astype(jnp.float32) / height
    for which, turns in enumerate(
        [
            (slope * across + shift_x) * place_freq,
            (tilt * along + shift_y) * line_freq,
            (slope * across) * place_freq,
        ]
    ):
        cosine, sine = cos_sin_turns(turns)
        phase_s[2 * which] = cosine
        phase_s[2 * which + 1] = sine

    def row_dft(real, imag):
        high, low = split_value(jnp.concatenate([real, imag], 0))
        table_high, table_low = row_ref[0], row_ref[1]
        out = mxu(high, table_high) + (mxu(low, table_high) + mxu(high, table_low))
        return (
            out[:rows, :wide] + out[rows:, wide:],
            out[rows:, :wide] - out[:rows, wide:],
        )

    def column_dft(real, imag):
        stacked = jnp.concatenate([real, imag], 1)
        stacked = jnp.concatenate(
            [stacked, jnp.zeros((tall - rows, 2 * wide), jnp.float32)], 0
        )
        high, low = split_value(stacked)

        def apply(which):
            table_high = column_ref[0, which, :rows]
            table_low = column_ref[1, which, :rows]
            return mxu(table_high, high) + (mxu(table_high, low) + mxu(table_low, high))

        by_cosine, by_sine = apply(0), apply(1)
        return (
            by_cosine[:, :wide] + by_sine[:, wide:],
            by_cosine[:, wide:] - by_sine[:, :wide],
        )

    def shear(dft, real, imag, which, sign):
        cosine = phase_s[2 * which]
        sine = phase_s[2 * which + 1]
        real, imag = dft(real, imag)
        turned = real * cosine + sign * (imag * sine)
        turned_negative = sign * (real * sine) - imag * cosine
        real, imag = dft(turned, turned_negative)
        return real, -imag

    real, imag = image_ref[0], image_ref[1]
    real, imag = shear(row_dft, real, imag, 0, 1.0)
    real, imag = shear(column_dft, real, imag, 1, 1.0)
    real, imag = shear(row_dft, real, imag, 2, 1.0)
    rotated_s[0] = real
    rotated_s[1] = imag

    weight = mask_ref[...].astype(jnp.float32)

    def masked(part, which):
        return (column_ref[part, which, :rows].astype(jnp.float32) * weight).astype(jnp.bfloat16)

    def triple(left, right):
        right_high, right_low = column_ref[0, right], column_ref[1, right]
        left_high, left_low = masked(0, left), masked(1, left)
        return mxu(left_high, right_high) + (
            mxu(left_low, right_high) + mxu(left_high, right_low)
        )

    table_real = triple(0, 0) + triple(1, 1)
    table_imag = triple(1, 0) - triple(0, 1)
    table_s[:rows, :tall] = table_real.astype(jnp.bfloat16)
    table_s[:rows, tall:] = (-table_imag).astype(jnp.bfloat16)
    table_s[rows:, :tall] = table_imag.astype(jnp.bfloat16)
    table_s[rows:, tall:] = table_real.astype(jnp.bfloat16)
    waved_s[...] = jnp.zeros_like(waved_s)
    sum_s[...] = jnp.zeros_like(sum_s)

    pair = 2 if coils % 2 == 0 else 1

    def some_coils(step, carry):
        for at in range(pair):
            coil = step * pair + at
            coil_real = coil_ref[coil, 0].astype(jnp.float32)
            coil_imag = coil_ref[coil, 1].astype(jnp.float32)
            real, imag = rotated_s[0], rotated_s[1]
            coil_image = jnp.concatenate(
                [
                    (coil_real * real - coil_imag * imag).astype(jnp.bfloat16),
                    (coil_real * imag + coil_imag * real).astype(jnp.bfloat16),
                ],
                1,
            )
            spectra = mxu(coil_image, pad_s[...])
            real, imag = spectra[:, :deep], spectra[:, deep:]
            cosine, sine = cosine_s[...], sine_s[...]
            columns = slice(at * deep, (at + 1) * deep)
            waved_s[:rows, columns] = (real * cosine - imag * sine).astype(jnp.bfloat16)
            waved_s[tall : tall + rows, columns] = (real * sine + imag * cosine).astype(
                jnp.bfloat16
            )
        for at in range(pair):
            coil = step * pair + at
            columns = slice(at * deep, (at + 1) * deep)
            projected = mxu(table_s[...], waved_s[:, columns])
            real, imag = projected[:rows], projected[rows:]
            cosine, sine = cosine_s[...], sine_s[...]
            unwaved_s[at, :, :deep] = (real * cosine + imag * sine).astype(jnp.bfloat16)
            unwaved_s[at, :, deep:] = (imag * cosine - real * sine).astype(jnp.bfloat16)
        for at in range(pair):
            coil = step * pair + at
            back = mxu(unwaved_s[at], crop_s[...])
            real, imag = back[:, :wide], back[:, wide:]
            coil_real = coil_ref[coil, 0].astype(jnp.float32)
            coil_imag = coil_ref[coil, 1].astype(jnp.float32)
            sum_s[0] += coil_real * real + coil_imag * imag
            sum_s[1] += coil_real * imag - coil_imag * real
        return carry

    lax.fori_loop(0, coils // pair, some_coils, 0)

    real, imag = sum_s[0], sum_s[1]
    real, imag = shear(row_dft, real, imag, 2, -1.0)
    real, imag = shear(column_dft, real, imag, 1, -1.0)
    real, imag = shear(row_dft, real, imag, 0, -1.0)
    out_ref[0] = real
    out_ref[1] = imag


def partner_kernel(own_ref, out_ref, other_s, send_sem, recv_sem):
    partner = {"shot": 1 - lax.axis_index("shot")}
    barrier = pltpu.get_barrier_semaphore()
    pl.semaphore_signal(
        barrier, inc=1, device_id=partner, device_id_type=pl.DeviceIdType.MESH
    )
    pl.semaphore_wait(barrier, 1)
    copy = pltpu.make_async_remote_copy(
        src_ref=own_ref,
        dst_ref=other_s,
        send_sem=send_sem,
        recv_sem=recv_sem,
        device_id=partner,
        device_id_type=pl.DeviceIdType.MESH,
    )
    copy.start()
    copy.wait()
    out_ref[...] = own_ref[...] + other_s[...]


def whole_slice(image, coil_maps, psf_phase, line_mask, motion):
    height, width, readout = image.shape[0], image.shape[2], psf_phase.shape[1]
    coils = coil_maps.shape[0]
    rows, wide = round_up(height, 16), round_up(width, 256)
    tall, deep = round_up(height, 256), round_up(readout, 128)
    edges = (0, rows - height, 0), (0, wide - width, 0)
    zero = jnp.zeros((), jnp.float32)
    planes = lax.pad(jnp.swapaxes(image, 0, 1), zero, ((0, 0, 0),) + edges)
    coil_planes = lax.pad(
        jnp.swapaxes(coil_maps, 1, 2),
        zero.astype(coil_maps.dtype),
        ((0, 0, 0), (0, 0, 0)) + edges,
    )
    mask = lax.pad(line_mask, jnp.int32(0), ((0, 0, 0), (0, tall - height, 0)))
    tables = [jnp.asarray(table) for table in host_tables(width, height, readout)]
    vmem = pl.BlockSpec(memory_space=pltpu.VMEM)
    own = pl.pallas_call(
        functools.partial(slice_kernel, height, width, readout),
        out_shape=jax.ShapeDtypeStruct((2, rows, wide), jnp.float32),
        in_specs=[pl.BlockSpec(memory_space=pltpu.SMEM)] + [vmem] * 8,
        out_specs=vmem,
        scratch_shapes=[
            pltpu.VMEM((2 * wide, 2 * deep), jnp.bfloat16),
            pltpu.VMEM((2 * deep, 2 * wide), jnp.bfloat16),
            pltpu.VMEM((rows, deep), jnp.float32),
            pltpu.VMEM((rows, deep), jnp.float32),
            pltpu.VMEM((2 * rows, 2 * tall), jnp.bfloat16),
            pltpu.VMEM((2 * tall, 2 * deep), jnp.bfloat16),
            pltpu.VMEM((2, rows, 2 * deep), jnp.bfloat16),
            pltpu.VMEM((2, rows, wide), jnp.float32),
            pltpu.VMEM((2, rows, wide), jnp.float32),
            pltpu.VMEM((6, rows, wide), jnp.float32),
        ],
        compiler_params=pltpu.CompilerParams(vmem_limit_bytes=60 * 1024 * 1024),
        name="slice_kernel",
    )(motion, mask, planes, coil_planes, psf_phase, *tables)
    both = pl.pallas_call(
        partner_kernel,
        out_shape=jax.ShapeDtypeStruct(own.shape, own.dtype),
        in_specs=[vmem],
        out_specs=vmem,
        scratch_shapes=[
            pltpu.VMEM(own.shape, own.dtype),
            pltpu.SemaphoreType.DMA,
            pltpu.SemaphoreType.DMA,
        ],
        compiler_params=pltpu.CompilerParams(collective_id=0, has_side_effects=True),
        name="partner_kernel",
    )(own)
    return jnp.swapaxes(both[:, :height, :width], 0, 1)


def on_device(image, coil_maps, psf_phase, line_mask, motion):
    lines = image.shape[0]
    width = image.shape[2]
    readout = psf_phase.shape[1]
    if lines == NY and lax.axis_size("shot") == 2:
        return whole_slice(image, coil_maps, psf_phase, line_mask, motion)
    devices = lax.axis_size("space")
    device_rank = lax.axis_index("space")
    pad_table = block(dft_parts(width, readout, readout, -1.0)).astype(jnp.bfloat16)
    crop_table = block(dft_parts(readout, width, readout, 1.0)).astype(jnp.bfloat16)
    group_size = max(1, NY // lines)
    bit_count = group_size.bit_length() - 1
    own_coils = regroup_coils(coil_maps, bit_count, device_rank)
    own_psf = gather_slice(psf_phase, bit_count, device_rank)
    projector = line_table(line_mask[0])
    rotated = rotate_shards(image, motion[0], 1, device_rank, devices)
    slab_image = gather_slice(rotated, bit_count, device_rank)
    waved = encode(own_coils, slab_image, own_psf, pad_table)
    partial_sum = decode(own_coils, project(projector, waved), own_psf, crop_table)
    combined = sum_slice(partial_sum, bit_count, device_rank)
    running = rotate_shards(combined, motion[0], -1, device_rank, devices)
    return lax.psum(running, "shot")


def solution(mesh):
    in_specs = (
        P(("parts", "space"), None, None),
        P(None, ("parts", "space"), None, None),
        P(("parts", "space"), None),
        P(("parts", "shot"), None),
        P(("parts", "shot"), None),
    )
    out_specs = P(("parts", "space"), None, None)
    return jax.shard_map(
        on_device, mesh=mesh, in_specs=in_specs, out_specs=out_specs, check_vma=False
    )
```

```python
import functools
import math

import jax
import jax.numpy as jnp
import numpy as np
from jax import lax
from jax.experimental import pallas as pl
from jax.experimental.pallas import tpu as pltpu
from jax.sharding import PartitionSpec as P

NY = 200
LEVELS = 17


PRECISE = lax.Precision.HIGHEST
ANGLE_STEP = 0.02
SHIFT_STEP = 0.5


def from_partner(value, axis, apart):
    mask = 2**apart
    pairs = [(source, source ^ mask) for source in range(lax.axis_size(axis))]
    return lax.ppermute(value, axis, pairs)


def dft_parts(size_in, size_out, modulus, sign):
    inputs = jnp.arange(size_in, dtype=jnp.int32)[:, None]
    outputs = jnp.arange(size_out, dtype=jnp.int32)[None, :]
    angle = (inputs * outputs % modulus).astype(jnp.float32) * (2.0 * jnp.pi / modulus)
    factor = float(modulus) ** (-0.5)
    return (jnp.cos(angle) * factor, jnp.sin(angle) * (sign * factor))


def block(parts):
    real_part, imag_part = parts
    upper = jnp.concatenate([real_part, imag_part], 1)
    bottom = jnp.concatenate([-imag_part, real_part], 1)
    return jnp.concatenate([upper, bottom], 0)


def quad(real_part, imag_part):
    return jnp.stack(
        [jnp.stack([real_part, -imag_part], 1), jnp.stack([imag_part, real_part], 1)], 0
    )


def signed_freq(length):
    counter = jnp.arange(length, dtype=jnp.int32)
    return jnp.where(counter < length // 2, counter, counter - length).astype(jnp.float32)


def turn_phase(values, phase):
    cosine = jnp.cos(phase)
    sine_part = jnp.sin(phase)
    real_part = values[..., 0, :]
    imag_part = values[..., 1, :]
    return jnp.stack(
        [real_part * cosine - imag_part * sine_part, real_part * sine_part + imag_part * cosine], -2
    )


def complex_mul(left, right):
    return jnp.stack(
        [
            left[..., 0, :] * right[..., 0, :] - left[..., 1, :] * right[..., 1, :],
            left[..., 0, :] * right[..., 1, :] + left[..., 1, :] * right[..., 0, :],
        ],
        -2,
    )


def conj_mul(left, right):
    return jnp.stack(
        [
            left[..., 0, :] * right[..., 0, :] + left[..., 1, :] * right[..., 1, :],
            left[..., 0, :] * right[..., 1, :] - left[..., 1, :] * right[..., 0, :],
        ],
        -2,
    )


def shear_rows(values, shift, sign):
    length = values.shape[-1]
    lines = values.shape[0]
    forward = block(dft_parts(length, length, length, -1.0))
    inverse = block(dft_parts(length, length, length, 1.0))
    spectra = jnp.dot(
        values.reshape(lines, 2 * length),
        forward,
        precision=PRECISE,
        preferred_element_type=jnp.float32,
    )
    phase = sign * -2.0 * jnp.pi / length * shift[:, None] * signed_freq(length)[None, :]
    spectra = turn_phase(spectra.reshape(lines, 2, length), phase)
    result = jnp.dot(
        spectra.reshape(lines, 2 * length),
        inverse,
        precision=PRECISE,
        preferred_element_type=jnp.float32,
    )
    return result.reshape(lines, 2, length)


def shear_columns(values, shift, sign):
    length = values.shape[1]
    forward = quad(*dft_parts(length, length, length, -1.0))
    inverse = quad(*dft_parts(length, length, length, 1.0))
    spectra = jnp.einsum("oaib,zbix->zaox", forward, values, precision=PRECISE)
    phase = sign * -2.0 * jnp.pi / length * signed_freq(length)[:, None] * shift[None, :]
    spectra = turn_phase(spectra, phase)
    return jnp.einsum("oaib,zbix->zaox", inverse, spectra, precision=PRECISE)


def geometry(motion_row):
    offsets = motion_row.astype(jnp.float32) - (LEVELS - 1) / 2.0
    angle = offsets[0] * ANGLE_STEP
    return (-jnp.tan(angle / 2.0), jnp.sin(angle), offsets[1] * SHIFT_STEP, offsets[2] * SHIFT_STEP)


def line_table(mask_row):
    cosine, sine_part = dft_parts(NY, NY, NY, 1.0)
    weight = mask_row.astype(jnp.float32)[:, None]
    real_part = jnp.dot(cosine.T, weight * cosine, precision=PRECISE) + jnp.dot(
        sine_part.T, weight * sine_part, precision=PRECISE
    )
    imag_part = jnp.dot(sine_part.T, weight * cosine, precision=PRECISE) - jnp.dot(
        cosine.T, weight * sine_part, precision=PRECISE
    )
    return quad(real_part, imag_part).astype(jnp.bfloat16)


def to_columns(values):
    return lax.all_to_all(values, "space", split_axis=2, concat_axis=0, tiled=True)


def to_rows(values):
    return lax.all_to_all(values, "space", split_axis=0, concat_axis=2, tiled=True)


def rotate_shards(values, motion_row, sign, device_rank, devices):
    slope, tilt, shift_x, shift_y = geometry(motion_row)
    lines = values.shape[0]
    width = values.shape[2]
    across = ((device_rank * lines + jnp.arange(lines, dtype=jnp.int32)) % NY).astype(
        jnp.float32
    ) - NY / 2.0

    def column_pass(current):
        columns = width // devices
        along = (device_rank * columns + jnp.arange(columns, dtype=jnp.int32)).astype(
            jnp.float32
        ) - width / 2.0
        gathered = to_columns(current)
        all_lines = gathered.shape[0]
        view_slices = gathered.reshape(all_lines // NY, NY, 2, columns)
        sheared = shear_columns(view_slices, tilt * along + shift_y, sign).reshape(
            all_lines, 2, columns
        )
        return to_rows(sheared)

    if sign > 0:
        current = shear_rows(values, slope * across + shift_x, 1.0)
        current = column_pass(current)
        return shear_rows(current, slope * across, 1.0)
    current = shear_rows(values, slope * across, -1.0)
    current = column_pass(current)
    return shear_rows(current, slope * across + shift_x, -1.0)


def gather_slice(values, bit_count, device_rank):
    for bit_index in range(bit_count):
        partner = from_partner(values, "space", bit_index)
        low_side = device_rank >> bit_index & 1 == 0
        values = jnp.where(
            low_side, jnp.concatenate([values, partner], 0), jnp.concatenate([partner, values], 0)
        )
    return values


def sum_slice(values, bit_count, device_rank):
    for bit_index in reversed(range(bit_count)):
        half_rows = values.shape[0] // 2
        low_side = device_rank >> bit_index & 1 == 0
        kept_part = jnp.where(low_side, values[:half_rows], values[half_rows:])
        sent_part = jnp.where(low_side, values[half_rows:], values[:half_rows])
        values = kept_part + from_partner(sent_part, "space", bit_index)
    return values


def regroup_coils(coil_maps, bit_count, device_rank):
    group_size = 1 << bit_count
    pieces = coil_maps.reshape((group_size, coil_maps.shape[0] // group_size) + coil_maps.shape[1:])
    for bit_index in range(bit_count):
        old_shape = pieces.shape
        halves = pieces.reshape((group_size >> bit_index + 1, 2, 1 << bit_index) + old_shape[1:])
        low_side = device_rank >> bit_index & 1 == 0
        kept_part = jnp.where(low_side, halves[:, 0], halves[:, 1])
        sent_part = jnp.where(low_side, halves[:, 1], halves[:, 0])
        partner = from_partner(sent_part, "space", bit_index)
        pieces = jnp.stack(
            [jnp.where(low_side, kept_part, partner), jnp.where(low_side, partner, kept_part)], 1
        ).reshape(old_shape)
    moved = jnp.moveaxis(pieces, 0, 1)
    return moved.reshape((moved.shape[0], group_size * coil_maps.shape[1]) + coil_maps.shape[2:])


def encode(coils, slab_image, psf_values, pad_table):
    coil_count, lines, _, width = coils.shape
    readout = psf_values.shape[1]
    coil_image = complex_mul(coils.astype(jnp.float32), slab_image[None]).astype(jnp.bfloat16)
    spectra = jnp.dot(
        coil_image.reshape(coil_count * lines, 2 * width),
        pad_table,
        preferred_element_type=jnp.float32,
    )
    return turn_phase(spectra.reshape(coil_count, lines, 2, readout), psf_values[None]).astype(
        jnp.bfloat16
    )


def project(projector, waved):
    coil_count, lines, _, columns = waved.shape
    view_slices = waved.reshape(coil_count, lines // NY, NY, 2, columns)
    projected = jnp.einsum(
        "oaib,czbik->czaok", projector, view_slices, preferred_element_type=jnp.float32
    )
    return projected.astype(jnp.bfloat16).reshape(waved.shape)


def decode(coils, projected, psf_values, crop_table):
    coil_count, lines, _, readout = projected.shape
    width = coils.shape[3]
    unwaved = turn_phase(projected.astype(jnp.float32), -psf_values[None]).astype(jnp.bfloat16)
    back = jnp.dot(
        unwaved.reshape(coil_count * lines, 2 * readout),
        crop_table,
        preferred_element_type=jnp.float32,
    )
    return jnp.sum(
        conj_mul(coils.astype(jnp.float32), back.reshape(coil_count, lines, 2, width)), 0
    )


def round_up(size, step):
    return -(-size // step) * step


def host_dft(size_in, size_out, modulus):
    turns = np.outer(np.arange(size_in), np.arange(size_out)) % modulus
    angle = turns.astype(np.float64) * (2.0 * np.pi / modulus)
    factor = float(modulus) ** -0.5
    return np.cos(angle) * factor, np.sin(angle) * factor


def placed(table, rows, columns):
    out = np.zeros((rows, columns), np.float64)
    out[: table.shape[0], : table.shape[1]] = table
    return out


def split_table(table):
    high = table.astype(np.float32).astype(jnp.bfloat16)
    low = (table - high.astype(np.float64)).astype(np.float32).astype(jnp.bfloat16)
    return np.stack([high, low])


def host_tables(width, height, readout):
    tall = round_up(height, 256)
    cosine, sine = host_dft(readout, width, readout)
    encode_table = np.block([[cosine, sine], [-sine, cosine]])
    row_parts = host_dft(width, width, width)
    column_parts = [placed(part, tall, tall) for part in host_dft(height, height, height)]
    return (
        encode_table.astype(np.float32).astype(jnp.bfloat16),
        encode_table.T.astype(np.float32).astype(jnp.bfloat16),
        split_table(np.concatenate(row_parts, 0)),
        split_table(np.concatenate(column_parts, 1)),
    )


SINE = [(-1.0) ** n / math.factorial(2 * n + 1) for n in range(6)]
COSINE = [(-1.0) ** n / math.factorial(2 * n) for n in range(7)]


def poly(square, coefficients):
    value = jnp.full_like(square, coefficients[-1])
    for coefficient in reversed(coefficients[:-1]):
        value = value * square + coefficient
    return value


def cos_sin_of_half(half):
    square = half * half
    sine = half * poly(square, SINE)
    cosine = poly(square, COSINE)
    return 1.0 - 2.0 * sine * sine, 2.0 * sine * cosine


def cos_sin_turns(turns):
    rest = turns - jnp.floor(turns + 0.5)
    return cos_sin_of_half(rest * math.pi)


def split_value(value):
    high = value.astype(jnp.bfloat16)
    return high, (value - high.astype(jnp.float32)).astype(jnp.bfloat16)


def mxu(left, right):
    return jnp.dot(left, right, preferred_element_type=jnp.float32)


def slice_kernel(
    motion_ref,
    mask_ref,
    image_ref,
    psf_ref,
    row_ref,
    column_ref,
    coil_hbm,
    encode_hbm,
    decode_hbm,
    out_ref,
    coil_s,
    encode_s,
    decode_s,
    psf_s,
    mask_s,
    cosine_s,
    sine_s,
    phase_s,
    image_s,
    table_s,
    coil_image_s,
    waved_s,
    unwaved_s,
    sum_s,
    copy_sems,
):
    _, width, height = image_ref.shape
    readout = psf_ref.shape[1]
    tall = column_ref.shape[1]
    coils = coil_s.shape[0]

    copies = [
        pltpu.make_async_copy(source, target, copy_sems.at[at])
        for at, (source, target) in enumerate(
            [(coil_hbm, coil_s), (encode_hbm, encode_s), (decode_hbm, decode_s)]
        )
    ]
    for copy in copies:
        copy.start()

    psf_s[...] = jnp.zeros_like(psf_s)
    psf_s[:height, :readout] = psf_ref[...]
    turned_psf = jnp.transpose(psf_s[...])[:readout]
    turn_cosine, turn_sine = cos_sin_of_half(turned_psf * 0.5)
    cosine_s[...] = turn_cosine
    sine_s[...] = turn_sine

    theta = (motion_ref[0, 0].astype(jnp.float32) - (LEVELS - 1) / 2.0) * ANGLE_STEP
    shift_x = (motion_ref[0, 1].astype(jnp.float32) - (LEVELS - 1) / 2.0) * SHIFT_STEP
    shift_y = (motion_ref[0, 2].astype(jnp.float32) - (LEVELS - 1) / 2.0) * SHIFT_STEP
    half = theta * 0.5
    half_square = half * half
    slope = -half * (
        1.0
        + half_square
        * (1.0 / 3.0 + half_square * (2.0 / 15.0 + half_square * (17.0 / 315.0)))
    )
    square = theta * theta
    tilt = theta * (
        1.0 - square * (1.0 / 6.0 - square * (1.0 / 120.0 - square * (1.0 / 5040.0)))
    )

    place = lax.broadcasted_iota(jnp.int32, (width, tall), 0)
    line = lax.broadcasted_iota(jnp.int32, (width, tall), 1)
    across = line.astype(jnp.float32) - height / 2.0
    along = place.astype(jnp.float32) - width / 2.0
    place_freq = jnp.where(place < width // 2, place, place - width).astype(jnp.float32) / width
    line_freq = jnp.where(line < height // 2, line, line - height).astype(jnp.float32) / height
    for which, turns in enumerate(
        [
            (slope * across + shift_x) * place_freq,
            (tilt * along + shift_y) * line_freq,
            (slope * across) * place_freq,
        ]
    ):
        cosine, sine = cos_sin_turns(turns)
        phase_s[2 * which] = cosine
        phase_s[2 * which + 1] = sine

    def row_dft(real, imag):
        high, low = split_value(jnp.concatenate([real, imag], 1))
        table_high, table_low = row_ref[0], row_ref[1]
        out = mxu(table_high, high) + (mxu(table_high, low) + mxu(table_low, high))
        return (
            out[:width, :tall] + out[width:, tall:],
            out[:width, tall:] - out[width:, :tall],
        )

    def column_dft(real, imag):
        high, low = split_value(jnp.concatenate([real, imag], 0))
        table_high, table_low = column_ref[0], column_ref[1]
        out = mxu(high, table_high) + (mxu(low, table_high) + mxu(high, table_low))
        return (
            out[:width, :tall] + out[width:, tall:],
            out[width:, :tall] - out[:width, tall:],
        )

    def shear(dft, real, imag, which, sign):
        cosine = phase_s[2 * which]
        sine = phase_s[2 * which + 1]
        real, imag = dft(real, imag)
        turned = real * cosine + sign * (imag * sine)
        turned_negative = sign * (real * sine) - imag * cosine
        real, imag = dft(turned, turned_negative)
        return real, -imag

    image_s[...] = jnp.zeros_like(image_s)
    image_s[:, :, :height] = image_ref[...]
    real, imag = image_s[0], image_s[1]
    real, imag = shear(row_dft, real, imag, 0, 1.0)
    real, imag = shear(column_dft, real, imag, 1, 1.0)
    real, imag = shear(row_dft, real, imag, 2, 1.0)
    image_s[0] = real
    image_s[1] = imag

    mask_s[...] = jnp.zeros_like(mask_s)
    mask_s[:, :height] = mask_ref[...].astype(jnp.float32)
    weight = mask_s[...]

    def table_part(part, which):
        return column_ref[part, :, which * tall : (which + 1) * tall]

    def masked(part, which):
        return (table_part(part, which).astype(jnp.float32) * weight).astype(jnp.bfloat16)

    def triple(left, right):
        right_high, right_low = table_part(0, right), table_part(1, right)
        left_high, left_low = masked(0, left), masked(1, left)
        return mxu(left_high, right_high) + (
            mxu(left_low, right_high) + mxu(left_high, right_low)
        )

    table_real = triple(0, 0) + triple(1, 1)
    table_imag = triple(1, 0) - triple(0, 1)
    table_s[:tall, :tall] = table_real.astype(jnp.bfloat16)
    table_s[:tall, tall:] = (-table_imag).astype(jnp.bfloat16)
    table_s[tall:, :tall] = table_imag.astype(jnp.bfloat16)
    table_s[tall:, tall:] = table_real.astype(jnp.bfloat16)
    coil_image_s[...] = jnp.zeros_like(coil_image_s)
    sum_s[...] = jnp.zeros_like(sum_s)
    for copy in copies:
        copy.wait()

    pair = coil_image_s.shape[0]

    def some_coils(step, carry):
        for at in range(pair):
            coil = step * pair + at
            coil_real = coil_s[coil, 0].astype(jnp.float32)
            coil_imag = coil_s[coil, 1].astype(jnp.float32)
            real, imag = image_s[0, :, :height], image_s[1, :, :height]
            coil_image_s[at, :width, :height] = (coil_real * real - coil_imag * imag).astype(
                jnp.bfloat16
            )
            coil_image_s[at, width:, :height] = (coil_real * imag + coil_imag * real).astype(
                jnp.bfloat16
            )
        for at in range(pair):
            spectra = mxu(encode_s[...], coil_image_s[at])
            real, imag = spectra[:readout], spectra[readout:]
            cosine, sine = cosine_s[...], sine_s[...]
            waved_s[at, :, :tall] = (real * cosine - imag * sine).astype(jnp.bfloat16)
            waved_s[at, :, tall:] = (real * sine + imag * cosine).astype(jnp.bfloat16)
        for at in range(pair):
            projected = mxu(waved_s[at], table_s[...])
            real, imag = projected[:, :tall], projected[:, tall:]
            cosine, sine = cosine_s[...], sine_s[...]
            unwaved_s[at, :readout] = (real * cosine + imag * sine).astype(jnp.bfloat16)
            unwaved_s[at, readout:] = (imag * cosine - real * sine).astype(jnp.bfloat16)
        for at in range(pair):
            coil = step * pair + at
            back = mxu(decode_s[...], unwaved_s[at])
            real, imag = back[:width, :height], back[width:, :height]
            coil_real = coil_s[coil, 0].astype(jnp.float32)
            coil_imag = coil_s[coil, 1].astype(jnp.float32)
            sum_s[0, :, :height] += coil_real * real + coil_imag * imag
            sum_s[1, :, :height] += coil_real * imag - coil_imag * real
        return carry

    lax.fori_loop(0, coils // pair, some_coils, 0)

    real, imag = sum_s[0], sum_s[1]
    real, imag = shear(row_dft, real, imag, 2, -1.0)
    real, imag = shear(column_dft, real, imag, 1, -1.0)
    real, imag = shear(row_dft, real, imag, 0, -1.0)
    out_ref[0] = real[:, :height]
    out_ref[1] = imag[:, :height]


def partner_kernel(own_ref, other_ref, send_sem, recv_sem):
    partner = {"shot": 1 - lax.axis_index("shot")}
    barrier = pltpu.get_barrier_semaphore()
    pl.semaphore_signal(
        barrier, inc=1, device_id=partner, device_id_type=pl.DeviceIdType.MESH
    )
    pl.semaphore_wait(barrier, 1)
    copy = pltpu.make_async_remote_copy(
        src_ref=own_ref,
        dst_ref=other_ref,
        send_sem=send_sem,
        recv_sem=recv_sem,
        device_id=partner,
        device_id_type=pl.DeviceIdType.MESH,
    )
    copy.start()
    copy.wait()


def whole_slice(image, coil_maps, psf_phase, line_mask, motion):
    height, width, readout = image.shape[0], image.shape[2], psf_phase.shape[1]
    coils = coil_maps.shape[0]
    tall = round_up(height, 256)
    pair = 2 if coils % 2 == 0 else 1
    planes = jnp.transpose(image, (1, 2, 0))
    coil_planes = jnp.transpose(coil_maps, (0, 2, 3, 1))
    encode_table, decode_table, row_table, column_table = [
        jnp.asarray(table) for table in host_tables(width, height, readout)
    ]
    vmem = pl.BlockSpec(memory_space=pltpu.VMEM)
    anywhere = pl.BlockSpec(memory_space=pl.ANY)
    own = pl.pallas_call(
        slice_kernel,
        out_shape=jax.ShapeDtypeStruct((2, width, height), jnp.float32),
        in_specs=[pl.BlockSpec(memory_space=pltpu.SMEM)] + [vmem] * 5 + [anywhere] * 3,
        out_specs=vmem,
        scratch_shapes=[
            pltpu.VMEM(coil_planes.shape, coil_planes.dtype),
            pltpu.VMEM(encode_table.shape, jnp.bfloat16),
            pltpu.VMEM(decode_table.shape, jnp.bfloat16),
            pltpu.VMEM((tall, round_up(readout, 128)), jnp.float32),
            pltpu.VMEM((1, tall), jnp.float32),
            pltpu.VMEM((readout, tall), jnp.float32),
            pltpu.VMEM((readout, tall), jnp.float32),
            pltpu.VMEM((6, width, tall), jnp.float32),
            pltpu.VMEM((2, width, tall), jnp.float32),
            pltpu.VMEM((2 * tall, 2 * tall), jnp.bfloat16),
            pltpu.VMEM((pair, 2 * width, tall), jnp.bfloat16),
            pltpu.VMEM((pair, readout, 2 * tall), jnp.bfloat16),
            pltpu.VMEM((pair, 2 * readout, tall), jnp.bfloat16),
            pltpu.VMEM((2, width, tall), jnp.float32),
            pltpu.SemaphoreType.DMA((3,)),
        ],
        compiler_params=pltpu.CompilerParams(vmem_limit_bytes=56 * 1024 * 1024),
        name="slice_kernel",
    )(
        motion,
        line_mask,
        planes,
        psf_phase,
        row_table,
        column_table,
        coil_planes,
        encode_table,
        decode_table,
    )
    other = pl.pallas_call(
        partner_kernel,
        out_shape=jax.ShapeDtypeStruct(own.shape, own.dtype),
        in_specs=[vmem],
        out_specs=vmem,
        scratch_shapes=[pltpu.SemaphoreType.DMA, pltpu.SemaphoreType.DMA],
        compiler_params=pltpu.CompilerParams(collective_id=0, has_side_effects=True),
        name="partner_kernel",
    )(own)
    return jnp.transpose(own + other, (2, 0, 1))


def on_device(image, coil_maps, psf_phase, line_mask, motion):
    lines = image.shape[0]
    width = image.shape[2]
    readout = psf_phase.shape[1]
    if lines == NY and lax.axis_size("shot") == 2:
        return whole_slice(image, coil_maps, psf_phase, line_mask, motion)
    devices = lax.axis_size("space")
    device_rank = lax.axis_index("space")
    pad_table = block(dft_parts(width, readout, readout, -1.0)).astype(jnp.bfloat16)
    crop_table = block(dft_parts(readout, width, readout, 1.0)).astype(jnp.bfloat16)
    group_size = max(1, NY // lines)
    bit_count = group_size.bit_length() - 1
    own_coils = regroup_coils(coil_maps, bit_count, device_rank)
    own_psf = gather_slice(psf_phase, bit_count, device_rank)
    projector = line_table(line_mask[0])
    rotated = rotate_shards(image, motion[0], 1, device_rank, devices)
    slab_image = gather_slice(rotated, bit_count, device_rank)
    waved = encode(own_coils, slab_image, own_psf, pad_table)
    partial_sum = decode(own_coils, project(projector, waved), own_psf, crop_table)
    combined = sum_slice(partial_sum, bit_count, device_rank)
    running = rotate_shards(combined, motion[0], -1, device_rank, devices)
    return lax.psum(running, "shot")


def solution(mesh):
    in_specs = (
        P(("parts", "space"), None, None),
        P(None, ("parts", "space"), None, None),
        P(("parts", "space"), None),
        P(("parts", "shot"), None),
        P(("parts", "shot"), None),
    )
    out_specs = P(("parts", "space"), None, None)
    return jax.shard_map(
        on_device, mesh=mesh, in_specs=in_specs, out_specs=out_specs, check_vma=False
    )
```

```python
import functools
import math

import jax
import jax.numpy as jnp
import numpy as np
from jax import lax
from jax.experimental import pallas as pl
from jax.experimental.pallas import tpu as pltpu
from jax.sharding import PartitionSpec as P

NY = 200
LEVELS = 17


PRECISE = lax.Precision.HIGHEST
ANGLE_STEP = 0.02
SHIFT_STEP = 0.5


def from_partner(value, axis, apart):
    mask = 2**apart
    pairs = [(source, source ^ mask) for source in range(lax.axis_size(axis))]
    return lax.ppermute(value, axis, pairs)


def dft_parts(size_in, size_out, modulus, sign):
    inputs = jnp.arange(size_in, dtype=jnp.int32)[:, None]
    outputs = jnp.arange(size_out, dtype=jnp.int32)[None, :]
    angle = (inputs * outputs % modulus).astype(jnp.float32) * (2.0 * jnp.pi / modulus)
    factor = float(modulus) ** (-0.5)
    return (jnp.cos(angle) * factor, jnp.sin(angle) * (sign * factor))


def block(parts):
    real_part, imag_part = parts
    upper = jnp.concatenate([real_part, imag_part], 1)
    bottom = jnp.concatenate([-imag_part, real_part], 1)
    return jnp.concatenate([upper, bottom], 0)


def quad(real_part, imag_part):
    return jnp.stack(
        [jnp.stack([real_part, -imag_part], 1), jnp.stack([imag_part, real_part], 1)], 0
    )


def signed_freq(length):
    counter = jnp.arange(length, dtype=jnp.int32)
    return jnp.where(counter < length // 2, counter, counter - length).astype(jnp.float32)


def turn_phase(values, phase):
    cosine = jnp.cos(phase)
    sine_part = jnp.sin(phase)
    real_part = values[..., 0, :]
    imag_part = values[..., 1, :]
    return jnp.stack(
        [real_part * cosine - imag_part * sine_part, real_part * sine_part + imag_part * cosine], -2
    )


def complex_mul(left, right):
    return jnp.stack(
        [
            left[..., 0, :] * right[..., 0, :] - left[..., 1, :] * right[..., 1, :],
            left[..., 0, :] * right[..., 1, :] + left[..., 1, :] * right[..., 0, :],
        ],
        -2,
    )


def conj_mul(left, right):
    return jnp.stack(
        [
            left[..., 0, :] * right[..., 0, :] + left[..., 1, :] * right[..., 1, :],
            left[..., 0, :] * right[..., 1, :] - left[..., 1, :] * right[..., 0, :],
        ],
        -2,
    )


def shear_rows(values, shift, sign):
    length = values.shape[-1]
    lines = values.shape[0]
    forward = block(dft_parts(length, length, length, -1.0))
    inverse = block(dft_parts(length, length, length, 1.0))
    spectra = jnp.dot(
        values.reshape(lines, 2 * length),
        forward,
        precision=PRECISE,
        preferred_element_type=jnp.float32,
    )
    phase = sign * -2.0 * jnp.pi / length * shift[:, None] * signed_freq(length)[None, :]
    spectra = turn_phase(spectra.reshape(lines, 2, length), phase)
    result = jnp.dot(
        spectra.reshape(lines, 2 * length),
        inverse,
        precision=PRECISE,
        preferred_element_type=jnp.float32,
    )
    return result.reshape(lines, 2, length)


def shear_columns(values, shift, sign):
    length = values.shape[1]
    forward = quad(*dft_parts(length, length, length, -1.0))
    inverse = quad(*dft_parts(length, length, length, 1.0))
    spectra = jnp.einsum("oaib,zbix->zaox", forward, values, precision=PRECISE)
    phase = sign * -2.0 * jnp.pi / length * signed_freq(length)[:, None] * shift[None, :]
    spectra = turn_phase(spectra, phase)
    return jnp.einsum("oaib,zbix->zaox", inverse, spectra, precision=PRECISE)


def geometry(motion_row):
    offsets = motion_row.astype(jnp.float32) - (LEVELS - 1) / 2.0
    angle = offsets[0] * ANGLE_STEP
    return (-jnp.tan(angle / 2.0), jnp.sin(angle), offsets[1] * SHIFT_STEP, offsets[2] * SHIFT_STEP)


def line_table(mask_row):
    cosine, sine_part = dft_parts(NY, NY, NY, 1.0)
    weight = mask_row.astype(jnp.float32)[:, None]
    real_part = jnp.dot(cosine.T, weight * cosine, precision=PRECISE) + jnp.dot(
        sine_part.T, weight * sine_part, precision=PRECISE
    )
    imag_part = jnp.dot(sine_part.T, weight * cosine, precision=PRECISE) - jnp.dot(
        cosine.T, weight * sine_part, precision=PRECISE
    )
    return quad(real_part, imag_part).astype(jnp.bfloat16)


def to_columns(values):
    return lax.all_to_all(values, "space", split_axis=2, concat_axis=0, tiled=True)


def to_rows(values):
    return lax.all_to_all(values, "space", split_axis=0, concat_axis=2, tiled=True)


def rotate_shards(values, motion_row, sign, device_rank, devices):
    slope, tilt, shift_x, shift_y = geometry(motion_row)
    lines = values.shape[0]
    width = values.shape[2]
    across = ((device_rank * lines + jnp.arange(lines, dtype=jnp.int32)) % NY).astype(
        jnp.float32
    ) - NY / 2.0

    def column_pass(current):
        columns = width // devices
        along = (device_rank * columns + jnp.arange(columns, dtype=jnp.int32)).astype(
            jnp.float32
        ) - width / 2.0
        gathered = to_columns(current)
        all_lines = gathered.shape[0]
        view_slices = gathered.reshape(all_lines // NY, NY, 2, columns)
        sheared = shear_columns(view_slices, tilt * along + shift_y, sign).reshape(
            all_lines, 2, columns
        )
        return to_rows(sheared)

    if sign > 0:
        current = shear_rows(values, slope * across + shift_x, 1.0)
        current = column_pass(current)
        return shear_rows(current, slope * across, 1.0)
    current = shear_rows(values, slope * across, -1.0)
    current = column_pass(current)
    return shear_rows(current, slope * across + shift_x, -1.0)


def gather_slice(values, bit_count, device_rank):
    for bit_index in range(bit_count):
        partner = from_partner(values, "space", bit_index)
        low_side = device_rank >> bit_index & 1 == 0
        values = jnp.where(
            low_side, jnp.concatenate([values, partner], 0), jnp.concatenate([partner, values], 0)
        )
    return values


def sum_slice(values, bit_count, device_rank):
    for bit_index in reversed(range(bit_count)):
        half_rows = values.shape[0] // 2
        low_side = device_rank >> bit_index & 1 == 0
        kept_part = jnp.where(low_side, values[:half_rows], values[half_rows:])
        sent_part = jnp.where(low_side, values[half_rows:], values[:half_rows])
        values = kept_part + from_partner(sent_part, "space", bit_index)
    return values


def regroup_coils(coil_maps, bit_count, device_rank):
    group_size = 1 << bit_count
    pieces = coil_maps.reshape((group_size, coil_maps.shape[0] // group_size) + coil_maps.shape[1:])
    for bit_index in range(bit_count):
        old_shape = pieces.shape
        halves = pieces.reshape((group_size >> bit_index + 1, 2, 1 << bit_index) + old_shape[1:])
        low_side = device_rank >> bit_index & 1 == 0
        kept_part = jnp.where(low_side, halves[:, 0], halves[:, 1])
        sent_part = jnp.where(low_side, halves[:, 1], halves[:, 0])
        partner = from_partner(sent_part, "space", bit_index)
        pieces = jnp.stack(
            [jnp.where(low_side, kept_part, partner), jnp.where(low_side, partner, kept_part)], 1
        ).reshape(old_shape)
    moved = jnp.moveaxis(pieces, 0, 1)
    return moved.reshape((moved.shape[0], group_size * coil_maps.shape[1]) + coil_maps.shape[2:])


def encode(coils, slab_image, psf_values, pad_table):
    coil_count, lines, _, width = coils.shape
    readout = psf_values.shape[1]
    coil_image = complex_mul(coils.astype(jnp.float32), slab_image[None]).astype(jnp.bfloat16)
    spectra = jnp.dot(
        coil_image.reshape(coil_count * lines, 2 * width),
        pad_table,
        preferred_element_type=jnp.float32,
    )
    return turn_phase(spectra.reshape(coil_count, lines, 2, readout), psf_values[None]).astype(
        jnp.bfloat16
    )


def project(projector, waved):
    coil_count, lines, _, columns = waved.shape
    view_slices = waved.reshape(coil_count, lines // NY, NY, 2, columns)
    projected = jnp.einsum(
        "oaib,czbik->czaok", projector, view_slices, preferred_element_type=jnp.float32
    )
    return projected.astype(jnp.bfloat16).reshape(waved.shape)


def decode(coils, projected, psf_values, crop_table):
    coil_count, lines, _, readout = projected.shape
    width = coils.shape[3]
    unwaved = turn_phase(projected.astype(jnp.float32), -psf_values[None]).astype(jnp.bfloat16)
    back = jnp.dot(
        unwaved.reshape(coil_count * lines, 2 * readout),
        crop_table,
        preferred_element_type=jnp.float32,
    )
    return jnp.sum(
        conj_mul(coils.astype(jnp.float32), back.reshape(coil_count, lines, 2, width)), 0
    )


def round_up(size, step):
    return -(-size // step) * step


def host_dft(size_in, size_out, modulus):
    turns = np.outer(np.arange(size_in), np.arange(size_out)) % modulus
    angle = turns.astype(np.float64) * (2.0 * np.pi / modulus)
    factor = float(modulus) ** -0.5
    return np.cos(angle) * factor, np.sin(angle) * factor


def placed(table, rows, columns):
    out = np.zeros((rows, columns), np.float64)
    out[: table.shape[0], : table.shape[1]] = table
    return out


def split_table(table):
    high = table.astype(np.float32).astype(jnp.bfloat16)
    low = (table - high.astype(np.float64)).astype(np.float32).astype(jnp.bfloat16)
    return np.stack([high, low])


def host_tables(width, height, readout):
    tall = round_up(height, 256)
    cosine, sine = host_dft(readout, width, readout)
    encode_table = np.block([[cosine, sine], [-sine, cosine]])
    row_parts = host_dft(width, width, width)
    column_parts = [placed(part, tall, tall) for part in host_dft(height, height, height)]
    return (
        encode_table.astype(np.float32).astype(jnp.bfloat16),
        encode_table.T.astype(np.float32).astype(jnp.bfloat16),
        split_table(np.concatenate(row_parts, 0)),
        split_table(np.concatenate(column_parts, 1)),
    )


SINE = [(-1.0) ** n / math.factorial(2 * n + 1) for n in range(6)]
COSINE = [(-1.0) ** n / math.factorial(2 * n) for n in range(7)]


def poly(square, coefficients):
    value = jnp.full_like(square, coefficients[-1])
    for coefficient in reversed(coefficients[:-1]):
        value = value * square + coefficient
    return value


def cos_sin_of_half(half):
    square = half * half
    sine = half * poly(square, SINE)
    cosine = poly(square, COSINE)
    return 1.0 - 2.0 * sine * sine, 2.0 * sine * cosine


def cos_sin_turns(turns):
    rest = turns - jnp.floor(turns + 0.5)
    return cos_sin_of_half(rest * math.pi)


def split_value(value):
    high = value.astype(jnp.bfloat16)
    return high, (value - high.astype(jnp.float32)).astype(jnp.bfloat16)


def mxu(left, right):
    return jnp.dot(left, right, preferred_element_type=jnp.float32)


def slice_kernel(
    motion_ref,
    mask_ref,
    image_ref,
    psf_ref,
    row_ref,
    column_ref,
    coil_hbm,
    encode_hbm,
    decode_hbm,
    out_ref,
    coil_s,
    encode_s,
    decode_s,
    psf_s,
    mask_s,
    cosine_s,
    sine_s,
    phase_s,
    image_s,
    table_s,
    coil_image_s,
    waved_s,
    unwaved_s,
    sum_s,
    other_s,
    copy_sems,
):
    _, width, height = image_ref.shape
    readout = psf_ref.shape[1]
    tall = column_ref.shape[1]
    coils = coil_s.shape[0]

    copies = [
        pltpu.make_async_copy(source, target, copy_sems.at[at])
        for at, (source, target) in enumerate(
            [(coil_hbm, coil_s), (encode_hbm, encode_s), (decode_hbm, decode_s)]
        )
    ]
    for copy in copies:
        copy.start()
    partner = {"shot": 1 - lax.axis_index("shot")}
    barrier = pltpu.get_barrier_semaphore()
    pl.semaphore_signal(
        barrier, inc=1, device_id=partner, device_id_type=pl.DeviceIdType.MESH
    )

    psf_s[...] = jnp.zeros_like(psf_s)
    psf_s[:height, :readout] = psf_ref[...]
    turned_psf = jnp.transpose(psf_s[...])[:readout]
    turn_cosine, turn_sine = cos_sin_of_half(turned_psf * 0.5)
    cosine_s[...] = turn_cosine
    sine_s[...] = turn_sine

    theta = (motion_ref[0, 0].astype(jnp.float32) - (LEVELS - 1) / 2.0) * ANGLE_STEP
    shift_x = (motion_ref[0, 1].astype(jnp.float32) - (LEVELS - 1) / 2.0) * SHIFT_STEP
    shift_y = (motion_ref[0, 2].astype(jnp.float32) - (LEVELS - 1) / 2.0) * SHIFT_STEP
    half = theta * 0.5
    half_square = half * half
    slope = -half * (
        1.0
        + half_square
        * (1.0 / 3.0 + half_square * (2.0 / 15.0 + half_square * (17.0 / 315.0)))
    )
    square = theta * theta
    tilt = theta * (
        1.0 - square * (1.0 / 6.0 - square * (1.0 / 120.0 - square * (1.0 / 5040.0)))
    )

    place = lax.broadcasted_iota(jnp.int32, (width, tall), 0)
    line = lax.broadcasted_iota(jnp.int32, (width, tall), 1)
    across = line.astype(jnp.float32) - height / 2.0
    along = place.astype(jnp.float32) - width / 2.0
    place_freq = jnp.where(place < width // 2, place, place - width).astype(jnp.float32) / width
    line_freq = jnp.where(line < height // 2, line, line - height).astype(jnp.float32) / height
    for which, turns in enumerate(
        [
            (slope * across + shift_x) * place_freq,
            (tilt * along + shift_y) * line_freq,
            (slope * across) * place_freq,
        ]
    ):
        cosine, sine = cos_sin_turns(turns)
        phase_s[2 * which] = cosine
        phase_s[2 * which + 1] = sine

    def row_dft(real, imag):
        high, low = split_value(jnp.concatenate([real, imag], 1))
        table_high, table_low = row_ref[0], row_ref[1]
        out = mxu(table_high, high) + (mxu(table_high, low) + mxu(table_low, high))
        return (
            out[:width, :tall] + out[width:, tall:],
            out[:width, tall:] - out[width:, :tall],
        )

    def column_dft(real, imag):
        high, low = split_value(jnp.concatenate([real, imag], 0))
        table_high, table_low = column_ref[0], column_ref[1]
        out = mxu(high, table_high) + (mxu(low, table_high) + mxu(high, table_low))
        return (
            out[:width, :tall] + out[width:, tall:],
            out[width:, :tall] - out[:width, tall:],
        )

    def shear(dft, real, imag, which, sign):
        cosine = phase_s[2 * which]
        sine = phase_s[2 * which + 1]
        real, imag = dft(real, imag)
        turned = real * cosine + sign * (imag * sine)
        turned_negative = sign * (real * sine) - imag * cosine
        real, imag = dft(turned, turned_negative)
        return real, -imag

    image_s[...] = jnp.zeros_like(image_s)
    image_s[:, :, :height] = image_ref[...]
    real, imag = image_s[0], image_s[1]
    real, imag = shear(row_dft, real, imag, 0, 1.0)
    real, imag = shear(column_dft, real, imag, 1, 1.0)
    real, imag = shear(row_dft, real, imag, 2, 1.0)
    image_s[0] = real
    image_s[1] = imag

    mask_s[...] = jnp.zeros_like(mask_s)
    mask_s[:, :height] = mask_ref[...].astype(jnp.float32)
    weight = mask_s[...]

    def table_part(part, which):
        return column_ref[part, :, which * tall : (which + 1) * tall]

    def masked(part, which):
        return (table_part(part, which).astype(jnp.float32) * weight).astype(jnp.bfloat16)

    def triple(left, right):
        right_high, right_low = table_part(0, right), table_part(1, right)
        left_high, left_low = masked(0, left), masked(1, left)
        return mxu(left_high, right_high) + (
            mxu(left_low, right_high) + mxu(left_high, right_low)
        )

    table_real = triple(0, 0) + triple(1, 1)
    table_imag = triple(1, 0) - triple(0, 1)
    table_s[:tall, :tall] = table_real.astype(jnp.bfloat16)
    table_s[:tall, tall:] = (-table_imag).astype(jnp.bfloat16)
    table_s[tall:, :tall] = table_imag.astype(jnp.bfloat16)
    table_s[tall:, tall:] = table_real.astype(jnp.bfloat16)
    coil_image_s[...] = jnp.zeros_like(coil_image_s)
    sum_s[...] = jnp.zeros_like(sum_s)
    for copy in copies:
        copy.wait()

    pair = coil_image_s.shape[0]

    def some_coils(step, carry):
        for at in range(pair):
            coil = step * pair + at
            coil_real = coil_s[coil, 0].astype(jnp.float32)
            coil_imag = coil_s[coil, 1].astype(jnp.float32)
            real, imag = image_s[0, :, :height], image_s[1, :, :height]
            coil_image_s[at, :width, :height] = (coil_real * real - coil_imag * imag).astype(
                jnp.bfloat16
            )
            coil_image_s[at, width:, :height] = (coil_real * imag + coil_imag * real).astype(
                jnp.bfloat16
            )
        for at in range(pair):
            spectra = mxu(encode_s[...], coil_image_s[at])
            real, imag = spectra[:readout], spectra[readout:]
            cosine, sine = cosine_s[...], sine_s[...]
            waved_s[at, :, :tall] = (real * cosine - imag * sine).astype(jnp.bfloat16)
            waved_s[at, :, tall:] = (real * sine + imag * cosine).astype(jnp.bfloat16)
        for at in range(pair):
            projected = mxu(waved_s[at], table_s[...])
            real, imag = projected[:, :tall], projected[:, tall:]
            cosine, sine = cosine_s[...], sine_s[...]
            unwaved_s[at, :readout] = (real * cosine + imag * sine).astype(jnp.bfloat16)
            unwaved_s[at, readout:] = (imag * cosine - real * sine).astype(jnp.bfloat16)
        for at in range(pair):
            coil = step * pair + at
            back = mxu(decode_s[...], unwaved_s[at])
            real, imag = back[:width, :height], back[width:, :height]
            coil_real = coil_s[coil, 0].astype(jnp.float32)
            coil_imag = coil_s[coil, 1].astype(jnp.float32)
            sum_s[0, :, :height] += coil_real * real + coil_imag * imag
            sum_s[1, :, :height] += coil_real * imag - coil_imag * real
        return carry

    lax.fori_loop(0, coils // pair, some_coils, 0)

    real, imag = sum_s[0], sum_s[1]
    real, imag = shear(row_dft, real, imag, 2, -1.0)
    real, imag = shear(column_dft, real, imag, 1, -1.0)
    real, imag = shear(row_dft, real, imag, 0, -1.0)
    sum_s[0] = real
    sum_s[1] = imag
    pl.semaphore_wait(barrier, 1)
    copy = pltpu.make_async_remote_copy(
        src_ref=sum_s,
        dst_ref=other_s,
        send_sem=copy_sems.at[3],
        recv_sem=copy_sems.at[4],
        device_id=partner,
        device_id_type=pl.DeviceIdType.MESH,
    )
    copy.start()
    copy.wait()
    out_ref[...] = (sum_s[...] + other_s[...])[:, :, :height]


def whole_slice(image, coil_maps, psf_phase, line_mask, motion):
    height, width, readout = image.shape[0], image.shape[2], psf_phase.shape[1]
    coils = coil_maps.shape[0]
    tall = round_up(height, 256)
    pair = 2 if coils % 2 == 0 else 1
    planes = jnp.transpose(image, (1, 2, 0))
    coil_planes = jnp.transpose(coil_maps, (0, 2, 3, 1))
    encode_table, decode_table, row_table, column_table = [
        jnp.asarray(table) for table in host_tables(width, height, readout)
    ]
    vmem = pl.BlockSpec(memory_space=pltpu.VMEM)
    anywhere = pl.BlockSpec(memory_space=pl.ANY)
    total = pl.pallas_call(
        slice_kernel,
        out_shape=jax.ShapeDtypeStruct((2, width, height), jnp.float32),
        in_specs=[pl.BlockSpec(memory_space=pltpu.SMEM)] + [vmem] * 5 + [anywhere] * 3,
        out_specs=vmem,
        scratch_shapes=[
            pltpu.VMEM(coil_planes.shape, coil_planes.dtype),
            pltpu.VMEM(encode_table.shape, jnp.bfloat16),
            pltpu.VMEM(decode_table.shape, jnp.bfloat16),
            pltpu.VMEM((tall, round_up(readout, 128)), jnp.float32),
            pltpu.VMEM((1, tall), jnp.float32),
            pltpu.VMEM((readout, tall), jnp.float32),
            pltpu.VMEM((readout, tall), jnp.float32),
            pltpu.VMEM((6, width, tall), jnp.float32),
            pltpu.VMEM((2, width, tall), jnp.float32),
            pltpu.VMEM((2 * tall, 2 * tall), jnp.bfloat16),
            pltpu.VMEM((pair, 2 * width, tall), jnp.bfloat16),
            pltpu.VMEM((pair, readout, 2 * tall), jnp.bfloat16),
            pltpu.VMEM((pair, 2 * readout, tall), jnp.bfloat16),
            pltpu.VMEM((2, width, tall), jnp.float32),
            pltpu.VMEM((2, width, tall), jnp.float32),
            pltpu.SemaphoreType.DMA((5,)),
        ],
        compiler_params=pltpu.CompilerParams(
            vmem_limit_bytes=56 * 1024 * 1024, collective_id=0, has_side_effects=True
        ),
        name="slice_kernel",
    )(
        motion,
        line_mask,
        planes,
        psf_phase,
        row_table,
        column_table,
        coil_planes,
        encode_table,
        decode_table,
    )
    return jnp.transpose(total, (2, 0, 1))


def on_device(image, coil_maps, psf_phase, line_mask, motion):
    lines = image.shape[0]
    width = image.shape[2]
    readout = psf_phase.shape[1]
    if lines == NY and lax.axis_size("shot") == 2:
        return whole_slice(image, coil_maps, psf_phase, line_mask, motion)
    devices = lax.axis_size("space")
    device_rank = lax.axis_index("space")
    pad_table = block(dft_parts(width, readout, readout, -1.0)).astype(jnp.bfloat16)
    crop_table = block(dft_parts(readout, width, readout, 1.0)).astype(jnp.bfloat16)
    group_size = max(1, NY // lines)
    bit_count = group_size.bit_length() - 1
    own_coils = regroup_coils(coil_maps, bit_count, device_rank)
    own_psf = gather_slice(psf_phase, bit_count, device_rank)
    projector = line_table(line_mask[0])
    rotated = rotate_shards(image, motion[0], 1, device_rank, devices)
    slab_image = gather_slice(rotated, bit_count, device_rank)
    waved = encode(own_coils, slab_image, own_psf, pad_table)
    partial_sum = decode(own_coils, project(projector, waved), own_psf, crop_table)
    combined = sum_slice(partial_sum, bit_count, device_rank)
    running = rotate_shards(combined, motion[0], -1, device_rank, devices)
    return lax.psum(running, "shot")


def solution(mesh):
    in_specs = (
        P(("parts", "space"), None, None),
        P(None, ("parts", "space"), None, None),
        P(("parts", "space"), None),
        P(("parts", "shot"), None),
        P(("parts", "shot"), None),
    )
    out_specs = P(("parts", "space"), None, None)
    return jax.shard_map(
        on_device, mesh=mesh, in_specs=in_specs, out_specs=out_specs, check_vma=False
    )
```
